32 devices in a mesh: tensor: 4 (over y, core), context: 8 (over z, x).
Axes of the slice: x: 2, y: 2, z: 4, core: 2. Of those that a mesh axis runs over, the one named last changes fastest.
Arguments:
- query_rows: bfloat16 [2048, 8192], P('context', 'tensor'), may hold values from -160 to 160, as said below
- key_rows: bfloat16 [2048, 1024], P('context'), may hold values from -5 to 5, as said below
- value_rows: bfloat16 [2048, 1024], P('context'), may hold values from -6 to 6
- doc_ids: int32 [2048], P('context'), may hold values from 0 to 3, never falling along the last dimension, each value on 1 to 1024 neighbouring positions
- out_weight: bfloat16 [8192, 8192], P('tensor'), may hold values from -0.09375 to 0.09375
Outputs:
- mixed: bfloat16 [2048, 8192], P('context', 'tensor')
The draws below stay inside these ranges and needn't reach their ends.
Inputs may be any that keep to these rules, and one draw needn't show every extreme that they name: `query_rows`: within the range given by the table of arrays. `key_rows`: within the range given by the table of arrays. `doc_ids`: document numbers never fall along the sequence; every document has 1 to 1024 tokens and one has exactly 1024.
All inputs are finite; a program needn't handle non-finite values.
Results may differ from the reference program's by a relative error of at most 0.015.
Values may be sent and summed in bfloat16 or wider, within the bound.
No kernel may reach another device: no remote copies, remote signals or barrier semaphores. Data moves between devices by JAX's collectives and lax.ppermute only.
A program may use at most 128 MiB of HBM per device.

```python
import math
import jax
import jax.numpy as jnp
import numpy as np
from jax import lax

D = 8192
H = 64
KVH = 8
HD = 128
TOK_DEV = 256
DOC_MOST = 1024
TOKENS = 2048
DOCS = 4
N_TENSOR = 4


def make_pairs(key):
    key_draw = jnp.clip(jax.random.normal(jax.random.fold_in(key, 101), (TOKENS, KVH, HD), jnp.float32), -5.0, 5.0)
    query_draw = jax.random.normal(jax.random.fold_in(key, 202), (TOKENS, H, HD), jnp.float32)
    return (query_draw.reshape(TOKENS, H * HD), key_draw.reshape(TOKENS, KVH * HD))


def draw_query_rows(key, part):
    return make_pairs(key)[0].astype(jnp.bfloat16)


def draw_key_rows(key, part):
    return make_pairs(key)[1].astype(jnp.bfloat16)


def raised(result, own_key, source, target, shards_of, factor):
    def block_of(position):
        return (jnp.arange(result.shape[position]) // (result.shape[position] // shards_of)).reshape((-1,) + (1,) * (result.ndim - 1 - position))

    near = jax.random.permutation(own_key, shards_of)[block_of(target)]
    second = (block_of(target) + shards_of // 2) % shards_of
    return jnp.where((block_of(source) == near) | (block_of(source) == second), factor * result, result)


def shard_levels(rng, shape, split, least, largest):
    def one(axis_at, parts):
        heights = jax.random.uniform(jax.random.fold_in(jax.random.fold_in(rng, 6), axis_at), (parts,), jnp.float32, least / len(split), largest / len(split))
        return jnp.repeat(jnp.exp(heights), shape[axis_at] // parts).reshape((-1,) + (1,) * (len(shape) - axis_at - 1))

    gain = one(*split[0])
    for cut in split[1:]:
        gain = gain * one(*cut)
    return gain


def profile(amount, total, reach, lean):
    portions = [(1 << 20) // math.isqrt(standing ** lean) + 1 for standing in range(2, amount + 1)]
    spare, holding = total - reach - (amount - 1), [1] * (amount - 1)
    while spare > 0:
        candidates = [i for i in range(amount - 1) if holding[i] < reach]
        mass, left = sum([portions[i] for i in candidates]), spare
        for i in candidates:
            extra = min(reach - holding[i], max(1, left * portions[i] // mass), spare)
            holding[i] = holding[i] + extra
            spare = spare - extra
    return np.array([reach] + holding)


def ragged(own_key, number_of, total, limit, lean):
    if number_of == 2:
        one = jax.random.randint(own_key, (), max(1, total - limit), min(limit, total - 1) + 1)
        return jnp.stack([one, total - one])
    lengths = jnp.asarray(profile(number_of, total, limit, lean), jnp.int32)
    twos = (number_of - 1) // 2
    source_of, receiver = lengths[1:1 + 2 * twos:2], lengths[2:2 + 2 * twos:2]
    slack = jnp.minimum(source_of - 1, limit - receiver)
    shifted = jax.random.randint(jax.random.fold_in(own_key, 1), (twos,), 0, 1 << 20) % (slack + 1)
    lengths = lengths.at[1:1 + 2 * twos:2].set(source_of - shifted).at[2:2 + 2 * twos:2].set(receiver + shifted)
    return lengths[jax.random.permutation(jax.random.fold_in(own_key, 2), number_of)]


def normal_values(rng, shape, deviation, limit, cuts=(), kind=jnp.bfloat16):
    values = jax.random.normal(rng, shape, jnp.float32) * deviation
    if len(cuts) > 0:
        values = shard_levels(rng, shape, cuts, -0.22, 0.18) * values
    return jnp.clip(values, min=-limit, max=limit).astype(kind)


def bell_draw_with(stream_key, extent, width, most, cuts, heavy, kind=jnp.bfloat16):
    values = width * jax.random.normal(stream_key, extent, jnp.float32)
    if cuts:
        values = values * shard_levels(stream_key, extent, cuts, -0.22, 0.18)
    return jnp.clip(raised(values, jax.random.fold_in(stream_key, 3), *heavy), -most, most).astype(kind)


def setup_inputs(seed: int = 0) -> dict:
    key_of = jax.random.split(jax.random.key(seed), 6)
    return {
        "query_rows": draw_query_rows(jax.random.fold_in(key_of[5], 71), 0),
        "key_rows": draw_key_rows(jax.random.fold_in(key_of[5], 71), 0),
        "value_rows": normal_values(key_of[2], (TOKENS, KVH * HD), 1.0, 6.0, ((0, 8),)),
        "doc_ids": jnp.searchsorted(jnp.cumsum(ragged(key_of[3], DOCS, TOKENS, DOC_MOST, 2)), jnp.arange(TOKENS), side="right").astype(jnp.int32),
        "out_weight": bell_draw_with(key_of[4], (H * HD, D), (H * HD) ** -0.5, 0.09375, ((0, 4),), (0, 1, 4, 2.0)),
    }


def reference(query_rows, key_rows, value_rows, doc_ids, out_weight):
    group_size = H // KVH
    key_span = DOC_MOST + TOK_DEV
    padded_keys = jnp.pad(key_rows, ((DOC_MOST, 0), (0, 0)))
    padded_values = jnp.pad(value_rows, ((DOC_MOST, 0), (0, 0)))
    padded_docs = jnp.pad(doc_ids, (DOC_MOST, 0), constant_values=-1)

    def one_block(block_index):
        first_row = (block_index * TOK_DEV).astype(jnp.int32)
        block_queries = lax.dynamic_slice_in_dim(query_rows, first_row, TOK_DEV, 0)
        block_queries = block_queries.astype(jnp.float32).reshape(TOK_DEV, KVH, group_size, HD)
        window_keys = lax.dynamic_slice_in_dim(padded_keys, first_row, key_span, 0)
        window_keys = window_keys.astype(jnp.float32).reshape(key_span, KVH, HD)
        window_values = lax.dynamic_slice_in_dim(padded_values, first_row, key_span, 0)
        window_values = window_values.astype(jnp.float32).reshape(key_span, KVH, HD)
        window_docs = lax.dynamic_slice_in_dim(padded_docs, first_row, key_span, 0)
        query_docs = lax.dynamic_slice_in_dim(doc_ids, first_row, TOK_DEV, 0)
        query_pos = first_row + jnp.arange(TOK_DEV, dtype=jnp.int32)
        key_pos = first_row - DOC_MOST + jnp.arange(key_span, dtype=jnp.int32)
        allowed = (key_pos[None, :] <= query_pos[:, None]) & (window_docs[None, :] == query_docs[:, None])
        scores = jnp.einsum("tkgd,skd->kgts", block_queries, window_keys) * (HD ** -0.5)
        scores = jnp.where(allowed, scores, -jnp.inf)
        highest = jnp.max(scores, axis=-1, keepdims=True)
        weights = jnp.where(allowed, jnp.exp(scores - highest), 0.0)
        totals = jnp.sum(weights, axis=-1)
        rounded = lax.optimization_barrier(weights.astype(jnp.bfloat16)).astype(jnp.float32)
        numer = jnp.einsum("kgts,skd->kgtd", rounded, window_values)
        attended = numer / totals[..., None]
        return attended.transpose(2, 0, 1, 3).reshape(TOK_DEV, H * HD).astype(jnp.bfloat16)

    blocks = lax.map(one_block, jnp.arange(TOKENS // TOK_DEV, dtype=jnp.int32))
    attended = blocks.reshape(TOKENS, H * HD)
    local_width = (H // N_TENSOR) * HD

    def add_group(index, running):
        first_col = (index * local_width).astype(jnp.int32)
        columns = lax.dynamic_slice_in_dim(attended, first_col, local_width, 1)
        weight_rows = lax.dynamic_slice_in_dim(out_weight, first_col, local_width, 0)
        partial_value = jnp.dot(columns, weight_rows, preferred_element_type=jnp.float32)
        rounded = lax.optimization_barrier(partial_value.astype(jnp.bfloat16)).astype(jnp.float32)
        return running + rounded

    mixed = lax.fori_loop(0, N_TENSOR, add_group, jnp.zeros((TOKENS, D), jnp.float32))
    return mixed.astype(jnp.bfloat16)
```

```python
import functools
import math

import jax
import jax.numpy as jnp
from jax import lax
from jax.experimental import pallas as pl
from jax.experimental.pallas import tpu as pltpu
from jax.sharding import PartitionSpec as P

H = 64
KVH = 8
HD = 128
DOC_MOST = 1024
NEG_BIG = -1e30
DOC_ROWS = 16
FOLD = HD ** (-0.5) * math.log2(math.e)


def attend_kernel(kv_count, per_kv, blocks, query_ref, docs_ref, *refs):
    kv_refs = refs[:blocks]
    out_ref, bias, key_t, value_x = refs[blocks:]
    rows = query_ref.shape[0]
    span = kv_refs[0].shape[0] - DOC_ROWS
    width = kv_count * HD
    query_docs = docs_ref[:, :1]
    lane = lax.broadcasted_iota(jnp.int32, (span, HD), 1)
    ones = jnp.where(lane == 0, 1.0, 0.0).astype(jnp.bfloat16)
    for n, kv in enumerate(kv_refs):
        key_docs = kv[span:span + DOC_ROWS, :span].astype(jnp.float32)[:1]
        same = query_docs == key_docs
        if n == 0:
            row = lax.broadcasted_iota(jnp.int32, (rows, span), 0)
            col = lax.broadcasted_iota(jnp.int32, (rows, span), 1)
            same = same & (col <= row)
        bias[:, n * span:(n + 1) * span] = jnp.where(same, 0.0, NEG_BIG)
        for g in range(kv_count):
            key_t[g, :, n * span:(n + 1) * span] = kv[:span, g * HD:(g + 1) * HD].T
            value_x[g, n * span:(n + 1) * span, :HD] = kv[:span, width + g * HD:width + (g + 1) * HD]
            value_x[g, n * span:(n + 1) * span, HD:] = ones

    for g in range(kv_count):
        def one_head(i, carry, g=g):
            at = pl.ds(pl.multiple_of((g * per_kv + i) * HD, HD), HD)
            scores = jnp.dot(query_ref[:, at], key_t[g], preferred_element_type=jnp.float32)
            scores = scores + bias[...]
            top = jnp.max(scores, axis=-1, keepdims=True)
            weights = jnp.exp2(scores * FOLD - top * FOLD).astype(jnp.bfloat16)
            both = jnp.dot(weights, value_x[g], preferred_element_type=jnp.float32)
            out_ref[:, at] = (both[:, :HD] / both[:, HD:HD + 1]).astype(jnp.bfloat16)
            return carry

        lax.fori_loop(0, per_kv, one_head, 0, unroll=2 if per_kv % 2 == 0 else 1)


def attend(query, docs, kvs, kv_count):
    rows = query.shape[0]
    per_kv = query.shape[1] // HD // kv_count
    blocks = len(kvs)
    span = kvs[0].shape[0] - DOC_ROWS
    keys = blocks * span
    heads = kv_count * per_kv
    whole = pl.BlockSpec(memory_space=pltpu.VMEM)
    return pl.pallas_call(
        functools.partial(attend_kernel, kv_count, per_kv, blocks),
        out_shape=jax.ShapeDtypeStruct(query.shape, jnp.bfloat16),
        in_specs=[whole] * (2 + blocks),
        out_specs=whole,
        scratch_shapes=[
            pltpu.VMEM((rows, keys), jnp.float32),
            pltpu.VMEM((kv_count, HD, keys), jnp.bfloat16),
            pltpu.VMEM((kv_count, keys, 2 * HD), jnp.bfloat16),
        ],
        compiler_params=pltpu.CompilerParams(vmem_limit_bytes=40 * 2**20),
        cost_estimate=pl.CostEstimate(
            flops=6 * heads * rows * keys * HD,
            bytes_accessed=4 * query.size + blocks * 2 * kvs[0].size,
            transcendentals=heads * rows * keys,
        ),
        name="attend",
    )(query, docs, *kvs)


def project_kernel(which_ref, left_ref, weight_ref, out_ref):
    out_ref[...] = jnp.dot(
        left_ref[...], weight_ref[...], preferred_element_type=jnp.float32
    ).astype(jnp.bfloat16)


def project(which, left, weight, width):
    rows, depth = left.shape
    tile = min(512, width)
    steps = width // tile
    return pl.pallas_call(
        project_kernel,
        out_shape=jax.ShapeDtypeStruct((rows, width), jnp.bfloat16),
        grid_spec=pltpu.PrefetchScalarGridSpec(
            num_scalar_prefetch=1,
            grid=(steps,),
            in_specs=[
                pl.BlockSpec((rows, depth), lambda j, w: (0, 0)),
                pl.BlockSpec((depth, tile), lambda j, w: (0, w[0] * steps + j)),
            ],
            out_specs=pl.BlockSpec((rows, tile), lambda j, w: (0, j)),
        ),
        compiler_params=pltpu.CompilerParams(vmem_limit_bytes=20 * 2**20),
        cost_estimate=pl.CostEstimate(
            flops=2 * rows * depth * width,
            bytes_accessed=2 * (depth * width + rows * width + rows * depth),
            transcendentals=0,
        ),
        name="project",
    )(which, left, weight)


def body(n_tensor, n_context, query_rows, key_rows, value_rows, doc_ids, out_weight):
    tokens_here = query_rows.shape[0]
    local_heads = query_rows.shape[1] // HD
    group_size = H // KVH
    kv_count = max(1, local_heads // group_size)
    tensor = lax.axis_index("tensor")
    first_kv = tensor * local_heads // group_size
    key_local = lax.dynamic_slice_in_dim(key_rows, first_kv * HD, kv_count * HD, 1)
    value_local = lax.dynamic_slice_in_dim(value_rows, first_kv * HD, kv_count * HD, 1)
    width = 2 * kv_count * HD
    docs = (doc_ids + 1).astype(jnp.float32)
    doc_rows = jnp.broadcast_to(
        jnp.pad(docs, (0, width - tokens_here)).astype(jnp.bfloat16)[None, :], (DOC_ROWS, width)
    )
    own = jnp.concatenate([jnp.concatenate([key_local, value_local], 1), doc_rows], 0)

    back = -(-(DOC_MOST - 1) // tokens_here)
    def up(x, by, only=None):
        pairs = [(i, i + by) for i in range(n_context) if 0 <= i + by < n_context]
        return lax.ppermute(x, "context", pairs)

    if back == 4 and n_context % 2 == 0:
        odd = lax.axis_index("context") % 2 == 1
        two = up(own, 2)
        below = lax.ppermute(own, "context", [(i, i + 1) for i in range(0, n_context, 2)])
        four = up(two, 2)
        beside = lax.ppermute(two, "context", [(i, i ^ 1) for i in range(n_context)])
        above = lax.ppermute(four, "context", [(i + 1, i) for i in range(0, n_context, 2)])
        kvs = [own, two, beside, four, jnp.where(odd, below, above)]
    else:
        kvs = [own] + [up(own, by) for by in range(1, min(back, n_context - 1) + 1)]

    query_docs = jnp.broadcast_to(docs[:, None], (tokens_here, HD))
    attended = attend(query_rows, query_docs, kvs, kv_count)

    columns = out_weight.shape[1] // n_tensor

    def reduced(rel, bit):
        if bit == 0:
            which = (tensor ^ rel).astype(jnp.int32).reshape(1)
            return project(which, attended, out_weight, columns)
        step = 1 << (bit - 1)
        sent = reduced(rel ^ step, bit - 1)
        got = lax.ppermute(sent, "tensor", [(i, i ^ step) for i in range(n_tensor)])
        mine = reduced(rel, bit - 1)
        return (mine.astype(jnp.float32) + got.astype(jnp.float32)).astype(jnp.bfloat16)

    return reduced(0, n_tensor.bit_length() - 1)


def solution(mesh):
    placed = (
        P("context", "tensor"),
        P("context", None),
        P("context", None),
        P("context"),
        P("tensor", None),
    )
    return jax.shard_map(
        functools.partial(body, mesh.shape["tensor"], mesh.shape["context"]),
        mesh=mesh,
        in_specs=placed,
        out_specs=P("context", "tensor"),
        check_vma=False,
    )
```

```python
import functools
import math

import jax
import jax.numpy as jnp
from jax import lax
from jax.experimental import pallas as pl
from jax.experimental.pallas import tpu as pltpu
from jax.sharding import PartitionSpec as P

H = 64
KVH = 8
HD = 128
DOC_MOST = 1024
NEG_BIG = -1e30
DOC_ROWS = 16
FOLD = HD ** (-0.5) * math.log2(math.e)


def attend_kernel(kv_count, per_kv, blocks, causal, carried, last, query_ref, docs_ref, *refs):
    kv_refs, refs = refs[:blocks], refs[blocks:]
    if carried:
        before_ref, refs = refs[0], refs[1:]
    if last:
        which_ref, weight_ref, refs = refs[0], refs[1], refs[2:]
    out_ref, refs = refs[0], refs[1:]
    if last:
        part_ref, refs = refs[0], refs[1:]
    bias, key_t, value_x = refs[:3]
    rows = query_ref.shape[0]
    span = kv_refs[0].shape[0] - DOC_ROWS
    width = kv_count * HD
    if last:
        held, sem = refs[3:]
        columns = held.shape[1]
        fetch = pltpu.make_async_copy(
            weight_ref.at[:, pl.ds(pl.multiple_of(which_ref[0] * columns, columns), columns)], held, sem
        )
        fetch.start()
    query_docs = docs_ref[:, :1]
    lane = lax.broadcasted_iota(jnp.int32, (span, HD), 1)
    ones = jnp.where(lane == 0, 1.0, 0.0).astype(jnp.bfloat16)
    for n, kv in enumerate(kv_refs):
        key_docs = kv[span:span + DOC_ROWS, :span].astype(jnp.float32)[:1]
        same = query_docs == key_docs
        if causal:
            row = lax.broadcasted_iota(jnp.int32, (rows, span), 0)
            col = lax.broadcasted_iota(jnp.int32, (rows, span), 1)
            same = same & (col <= row)
        bias[:, n * span:(n + 1) * span] = jnp.where(same, 0.0, NEG_BIG)
        for g in range(kv_count):
            key_t[g, :, n * span:(n + 1) * span] = kv[:span, g * HD:(g + 1) * HD].T
            value_x[g, n * span:(n + 1) * span, :HD] = kv[:span, width + g * HD:width + (g + 1) * HD]
            value_x[g, n * span:(n + 1) * span, HD:] = ones

    stat = lax.broadcasted_iota(jnp.int32, (rows, HD), 1)
    for g in range(kv_count):
        def one_head(i, carry, g=g):
            head = g * per_kv + i
            at = pl.ds(pl.multiple_of(head * HD, HD), HD)
            scores = jnp.dot(query_ref[:, at], key_t[g], preferred_element_type=jnp.float32)
            scores = scores + bias[...]
            top = jnp.max(scores, axis=-1, keepdims=True)
            if carried:
                old_top = before_ref[head, :, HD + 1:HD + 2]
                top = jnp.maximum(top, old_top)
            weights = jnp.exp2(scores * FOLD - top * FOLD).astype(jnp.bfloat16)
            both = jnp.dot(weights, value_x[g], preferred_element_type=jnp.float32)
            numer, total = both[:, :HD], both[:, HD:]
            if carried:
                fade = jnp.exp2(old_top * FOLD - top * FOLD)
                numer = numer + fade * before_ref[head, :, :HD]
                total = total + fade * before_ref[head, :, HD:]
            if last:
                out_ref[:, at] = (numer / total[:, :1]).astype(jnp.bfloat16)
            else:
                out_ref[head, :, :HD] = numer
                out_ref[head, :, HD:] = jnp.where(stat == 1, top, total)
            return carry

        lax.fori_loop(0, per_kv, one_head, 0, unroll=4 if per_kv % 4 == 0 else 1)
    if last:
        fetch.wait()
        part_ref[...] = jnp.dot(
            out_ref[...], held[...], preferred_element_type=jnp.float32
        ).astype(jnp.bfloat16)


def attend(query, docs, kvs, kv_count, causal=False, before=None, last=None):
    rows = query.shape[0]
    heads = query.shape[1] // HD
    per_kv = heads // kv_count
    blocks = len(kvs)
    keys = blocks * (kvs[0].shape[0] - DOC_ROWS)
    whole = pl.BlockSpec(memory_space=pltpu.VMEM)
    scratch = [
        pltpu.VMEM((rows, keys), jnp.float32),
        pltpu.VMEM((kv_count, HD, keys), jnp.bfloat16),
        pltpu.VMEM((kv_count, keys, 2 * HD), jnp.bfloat16),
    ]
    args, specs = [query, docs, *kvs], [whole] * (2 + blocks)
    if before is not None:
        args, specs = args + [before], specs + [whole]
    flops = 6 * heads * rows * keys * HD
    if last is None:
        outs = jax.ShapeDtypeStruct((heads, rows, 2 * HD), jnp.float32)
        out_specs = whole
    else:
        which, weight, columns = last
        args = args + [which, weight]
        specs = specs + [pl.BlockSpec(memory_space=pltpu.SMEM), pl.BlockSpec(memory_space=pl.ANY)]
        outs = (
            jax.ShapeDtypeStruct(query.shape, jnp.bfloat16),
            jax.ShapeDtypeStruct((rows, columns), jnp.bfloat16),
        )
        out_specs = (whole, whole)
        scratch += [pltpu.VMEM((weight.shape[0], columns), jnp.bfloat16), pltpu.SemaphoreType.DMA]
        flops += 2 * rows * query.shape[1] * columns
    return pl.pallas_call(
        functools.partial(
            attend_kernel, kv_count, per_kv, blocks, causal, before is not None, last is not None
        ),
        out_shape=outs,
        in_specs=specs,
        out_specs=out_specs,
        scratch_shapes=scratch,
        compiler_params=pltpu.CompilerParams(vmem_limit_bytes=44 * 2**20),
        cost_estimate=pl.CostEstimate(
            flops=flops,
            bytes_accessed=4 * query.size + blocks * 2 * kvs[0].size,
            transcendentals=heads * rows * keys,
        ),
        name="attend",
    )(*args)


def project_kernel(which_ref, left_ref, weight_ref, out_ref):
    out_ref[...] = jnp.dot(
        left_ref[...], weight_ref[...], preferred_element_type=jnp.float32
    ).astype(jnp.bfloat16)


def project(which, left, weight, width):
    rows, depth = left.shape
    tile = min(1024, width)
    steps = width // tile
    return pl.pallas_call(
        project_kernel,
        out_shape=jax.ShapeDtypeStruct((rows, width), jnp.bfloat16),
        grid_spec=pltpu.PrefetchScalarGridSpec(
            num_scalar_prefetch=1,
            grid=(steps,),
            in_specs=[
                pl.BlockSpec((rows, depth), lambda j, w: (0, 0)),
                pl.BlockSpec((depth, tile), lambda j, w: (0, w[0] * steps + j)),
            ],
            out_specs=pl.BlockSpec((rows, tile), lambda j, w: (0, j)),
        ),
        compiler_params=pltpu.CompilerParams(vmem_limit_bytes=24 * 2**20),
        cost_estimate=pl.CostEstimate(
            flops=2 * rows * depth * width,
            bytes_accessed=2 * (depth * width + rows * width + rows * depth),
            transcendentals=0,
        ),
        name="project",
    )(which, left, weight)


def body(n_tensor, n_context, query_rows, key_rows, value_rows, doc_ids, out_weight):
    tokens_here = query_rows.shape[0]
    local_heads = query_rows.shape[1] // HD
    group_size = H // KVH
    kv_count = max(1, local_heads // group_size)
    tensor = lax.axis_index("tensor")
    first_kv = tensor * local_heads // group_size
    key_local = lax.dynamic_slice_in_dim(key_rows, first_kv * HD, kv_count * HD, 1)
    value_local = lax.dynamic_slice_in_dim(value_rows, first_kv * HD, kv_count * HD, 1)
    width = 2 * kv_count * HD
    docs = (doc_ids + 1).astype(jnp.float32)
    doc_rows = jnp.broadcast_to(
        jnp.pad(docs, (0, width - tokens_here)).astype(jnp.bfloat16)[None, :], (DOC_ROWS, width)
    )
    own = jnp.concatenate([jnp.concatenate([key_local, value_local], 1), doc_rows], 0)

    back = -(-(DOC_MOST - 1) // tokens_here)
    def up(x, by, only=None):
        pairs = [(i, i + by) for i in range(n_context) if 0 <= i + by < n_context]
        return lax.ppermute(x, "context", pairs)

    columns = out_weight.shape[1] // n_tensor

    def chosen(rel):
        return (tensor ^ rel).astype(jnp.int32).reshape(1)

    query_docs = jnp.broadcast_to(docs[:, None], (tokens_here, HD))
    far = n_tensor - 1
    last = (chosen(far), out_weight, columns)
    if back == 4 and n_context % 2 == 0:
        odd = lax.axis_index("context") % 2 == 1
        two = up(own, 2)
        below = lax.ppermute(own, "context", [(i, i + 1) for i in range(0, n_context, 2)])
        state = attend(query_rows, query_docs, [own], kv_count, causal=True)
        two, below, state = lax.optimization_barrier((two, below, state))
        four = up(two, 2)
        beside = lax.ppermute(two, "context", [(i, i ^ 1) for i in range(n_context)])
        state = attend(query_rows, query_docs, [two], kv_count, before=state)
        four, beside, state = lax.optimization_barrier((four, beside, state))
        above = lax.ppermute(four, "context", [(i + 1, i) for i in range(0, n_context, 2)])
        kvs = [beside, four, jnp.where(odd, below, above)]
    else:
        state = attend(query_rows, query_docs, [own], kv_count, causal=True)
        kvs = [up(own, by) for by in range(1, min(back, n_context - 1) + 1)]
    attended, first_part = attend(
        query_rows, query_docs, kvs, kv_count, before=state, last=last
    )

    def reduced(rel, bit):
        nonlocal attended
        if bit == 0:
            if rel == far:
                return first_part
            return project(chosen(rel), attended, out_weight, columns)
        step = 1 << (bit - 1)
        sent = reduced(rel ^ step, bit - 1)
        attended, sent = lax.optimization_barrier((attended, sent))
        got = lax.ppermute(sent, "tensor", [(i, i ^ step) for i in range(n_tensor)])
        mine = reduced(rel, bit - 1)
        return (mine.astype(jnp.float32) + got.astype(jnp.float32)).astype(jnp.bfloat16)

    return reduced(0, n_tensor.bit_length() - 1)


def solution(mesh):
    placed = (
        P("context", "tensor"),
        P("context", None),
        P("context", None),
        P("context"),
        P("tensor", None),
    )
    return jax.shard_map(
        functools.partial(body, mesh.shape["tensor"], mesh.shape["context"]),
        mesh=mesh,
        in_specs=placed,
        out_specs=P("context", "tensor"),
        check_vma=False,
    )
```

```python
import functools
import math

import jax
import jax.numpy as jnp
from jax import lax
from jax.experimental import pallas as pl
from jax.experimental.pallas import tpu as pltpu
from jax.sharding import PartitionSpec as P

H = 64
KVH = 8
HD = 128
DOC_MOST = 1024
NEG_BIG = -1e30
DOC_ROWS = 16
FOLD = HD ** (-0.5) * math.log2(math.e)


def attend_kernel(kv_count, per_kv, blocks, causal, carried, last, query_ref, docs_ref, *refs):
    kv_refs, refs = refs[:blocks], refs[blocks:]
    if carried:
        before_ref, refs = refs[0], refs[1:]
    if last:
        which_ref, weight_ref, refs = refs[0], refs[1], refs[2:]
    out_ref, refs = refs[0], refs[1:]
    part_ref, refs = refs[0], refs[1:]
    if not last:
        part_ref[...] = docs_ref[...]
    bias, key_t, value_x = refs[:3]
    rows = query_ref.shape[0]
    span = kv_refs[0].shape[0] - DOC_ROWS
    width = kv_count * HD
    if last:
        held, sem = refs[3:]
        columns = held.shape[1]
        fetch = pltpu.make_async_copy(
            weight_ref.at[:, pl.ds(pl.multiple_of(which_ref[0] * columns, columns), columns)], held, sem
        )
        fetch.start()
    query_docs = docs_ref[:, :1]
    lane = lax.broadcasted_iota(jnp.int32, (span, HD), 1)
    ones = jnp.where(lane == 0, 1.0, 0.0).astype(jnp.bfloat16)
    for n, kv in enumerate(kv_refs):
        key_docs = kv[span:span + DOC_ROWS, :span].astype(jnp.float32)[:1]
        same = query_docs == key_docs
        if causal and n == 0:
            row = lax.broadcasted_iota(jnp.int32, (rows, span), 0)
            col = lax.broadcasted_iota(jnp.int32, (rows, span), 1)
            same = same & (col <= row)
        bias[:, n * span:(n + 1) * span] = jnp.where(same, 0.0, NEG_BIG)
        for g in range(kv_count):
            key_t[g, :, n * span:(n + 1) * span] = kv[:span, g * HD:(g + 1) * HD].T
            value_x[g, n * span:(n + 1) * span, :HD] = kv[:span, width + g * HD:width + (g + 1) * HD]
            value_x[g, n * span:(n + 1) * span, HD:] = ones

    stat = lax.broadcasted_iota(jnp.int32, (rows, HD), 1)
    for g in range(kv_count):
        def one_head(i, carry, g=g):
            head = g * per_kv + i
            at = pl.ds(pl.multiple_of(head * HD, HD), HD)
            scores = jnp.dot(query_ref[:, at], key_t[g], preferred_element_type=jnp.float32)
            scores = scores + bias[...]
            top = jnp.max(scores, axis=-1, keepdims=True)
            if carried:
                old_top = before_ref[head, :, HD + 1:HD + 2]
                top = jnp.maximum(top, old_top)
            weights = jnp.exp2(scores * FOLD - top * FOLD).astype(jnp.bfloat16)
            both = jnp.dot(weights, value_x[g], preferred_element_type=jnp.float32)
            numer, total = both[:, :HD], both[:, HD:]
            if carried:
                fade = jnp.exp2(old_top * FOLD - top * FOLD)
                numer = numer + fade * before_ref[head, :, :HD]
                total = total + fade * before_ref[head, :, HD:]
            if last:
                out_ref[:, at] = (numer / total[:, :1]).astype(jnp.bfloat16)
            else:
                out_ref[head, :, :HD] = numer
                out_ref[head, :, HD:] = jnp.where(stat == 1, top, total)
            return carry

        lax.fori_loop(0, per_kv, one_head, 0, unroll=4 if per_kv % 4 == 0 else 1)
    if last:
        fetch.wait()
        part_ref[...] = jnp.dot(
            out_ref[...], held[...], preferred_element_type=jnp.float32
        ).astype(jnp.bfloat16)


def attend(query, docs, kvs, kv_count, causal=False, before=None, last=None):
    rows = query.shape[0]
    heads = query.shape[1] // HD
    per_kv = heads // kv_count
    blocks = len(kvs)
    keys = blocks * (kvs[0].shape[0] - DOC_ROWS)
    whole = pl.BlockSpec(memory_space=pltpu.VMEM)
    scratch = [
        pltpu.VMEM((rows, keys), jnp.float32),
        pltpu.VMEM((kv_count, HD, keys), jnp.bfloat16),
        pltpu.VMEM((kv_count, keys, 2 * HD), jnp.bfloat16),
    ]
    args, specs = [query, docs, *kvs], [whole] * (2 + blocks)
    if before is not None:
        args, specs = args + [before], specs + [whole]
    flops = 6 * heads * rows * keys * HD
    if last is None:
        outs = (
            jax.ShapeDtypeStruct((heads, rows, 2 * HD), jnp.float32),
            jax.ShapeDtypeStruct(docs.shape, docs.dtype),
        )
    else:
        which, weight, columns = last
        args = args + [which, weight]
        specs = specs + [pl.BlockSpec(memory_space=pltpu.SMEM), pl.BlockSpec(memory_space=pl.ANY)]
        outs = (
            jax.ShapeDtypeStruct(query.shape, jnp.bfloat16),
            jax.ShapeDtypeStruct((rows, columns), jnp.bfloat16),
        )
        scratch += [pltpu.VMEM((weight.shape[0], columns), jnp.bfloat16), pltpu.SemaphoreType.DMA]
        flops += 2 * rows * query.shape[1] * columns
    return pl.pallas_call(
        functools.partial(
            attend_kernel, kv_count, per_kv, blocks, causal, before is not None, last is not None
        ),
        out_shape=outs,
        in_specs=specs,
        out_specs=(whole, whole),
        scratch_shapes=scratch,
        compiler_params=pltpu.CompilerParams(vmem_limit_bytes=(16 if last is None else 28) * 2**20),
        cost_estimate=pl.CostEstimate(
            flops=flops,
            bytes_accessed=4 * query.size + blocks * 2 * kvs[0].size,
            transcendentals=heads * rows * keys,
        ),
        name="attend",
    )(*args)


def project_kernel(which_ref, left_ref, weight_ref, out_ref):
    out_ref[...] = jnp.dot(
        left_ref[...], weight_ref[...], preferred_element_type=jnp.float32
    ).astype(jnp.bfloat16)


def project(which, left, weight, width):
    rows, depth = left.shape
    tile = min(1024, width)
    steps = width // tile
    return pl.pallas_call(
        project_kernel,
        out_shape=jax.ShapeDtypeStruct((rows, width), jnp.bfloat16),
        grid_spec=pltpu.PrefetchScalarGridSpec(
            num_scalar_prefetch=1,
            grid=(steps,),
            in_specs=[
                pl.BlockSpec((rows, depth), lambda j, w: (0, 0)),
                pl.BlockSpec((depth, tile), lambda j, w: (0, w[0] * steps + j)),
            ],
            out_specs=pl.BlockSpec((rows, tile), lambda j, w: (0, j)),
        ),
        compiler_params=pltpu.CompilerParams(vmem_limit_bytes=24 * 2**20),
        cost_estimate=pl.CostEstimate(
            flops=rows * depth * width // 4,
            bytes_accessed=2 * (depth * width + rows * width + rows * depth),
            transcendentals=0,
        ),
        name="project",
    )(which, left, weight)


def body(n_tensor, n_context, query_rows, key_rows, value_rows, doc_ids, out_weight):
    tokens_here = query_rows.shape[0]
    local_heads = query_rows.shape[1] // HD
    group_size = H // KVH
    kv_count = max(1, local_heads // group_size)
    tensor = lax.axis_index("tensor")
    first_kv = tensor * local_heads // group_size
    key_local = lax.dynamic_slice_in_dim(key_rows, first_kv * HD, kv_count * HD, 1)
    value_local = lax.dynamic_slice_in_dim(value_rows, first_kv * HD, kv_count * HD, 1)
    width = 2 * kv_count * HD
    docs = (doc_ids + 1).astype(jnp.float32)
    doc_rows = jnp.broadcast_to(
        jnp.pad(docs, (0, width - tokens_here)).astype(jnp.bfloat16)[None, :], (DOC_ROWS, width)
    )
    own = jnp.concatenate([jnp.concatenate([key_local, value_local], 1), doc_rows], 0)

    back = -(-(DOC_MOST - 1) // tokens_here)
    def up(x, by, only=None):
        pairs = [(i, i + by) for i in range(n_context) if 0 <= i + by < n_context]
        return lax.ppermute(x, "context", pairs)

    columns = out_weight.shape[1] // n_tensor

    def chosen(rel):
        return (tensor ^ rel).astype(jnp.int32).reshape(1)

    query_docs = jnp.broadcast_to(docs[:, None], (tokens_here, HD))
    far = n_tensor - 1
    last = (chosen(far), out_weight, columns)
    if back == 4 and n_context % 2 == 0:
        odd = lax.axis_index("context") % 2 == 1
        two = up(own, 2)
        below = lax.ppermute(own, "context", [(i, i + 1) for i in range(0, n_context, 2)])
        two, below = lax.optimization_barrier((two, below))
        four = up(two, 2)
        beside = lax.ppermute(two, "context", [(i, i ^ 1) for i in range(n_context)])
        state, query_docs = attend(query_rows, query_docs, [own, two], kv_count, causal=True)
        four, beside, query_docs = lax.optimization_barrier((four, beside, query_docs))
        above = lax.ppermute(four, "context", [(i + 1, i) for i in range(0, n_context, 2)])
        state, query_docs = attend(query_rows, query_docs, [beside, four], kv_count, before=state)
        kvs = [jnp.where(odd, below, above)]
    else:
        state, query_docs = attend(query_rows, query_docs, [own], kv_count, causal=True)
        kvs = [up(own, by) for by in range(1, min(back, n_context - 1) + 1)]
    attended, first_part = attend(
        query_rows, query_docs, kvs, kv_count, before=state, last=last
    )

    def reduced(rel, bit):
        nonlocal attended
        if bit == 0:
            if rel == far:
                return first_part
            return project(chosen(rel), attended, out_weight, columns)
        step = 1 << (bit - 1)
        sent = reduced(rel ^ step, bit - 1)
        attended, sent = lax.optimization_barrier((attended, sent))
        got = lax.ppermute(sent, "tensor", [(i, i ^ step) for i in range(n_tensor)])
        mine = reduced(rel, bit - 1)
        return (mine.astype(jnp.float32) + got.astype(jnp.float32)).astype(jnp.bfloat16)

    return reduced(0, n_tensor.bit_length() - 1)


def solution(mesh):
    placed = (
        P("context", "tensor"),
        P("context", None),
        P("context", None),
        P("context"),
        P("tensor", None),
    )
    return jax.shard_map(
        functools.partial(body, mesh.shape["tensor"], mesh.shape["context"]),
        mesh=mesh,
        in_specs=placed,
        out_specs=P("context", "tensor"),
        check_vma=False,
    )
```
